16 devices in a mesh: dep: 2 (over z), col: 2 (over y), row: 4 (over x, core).
Axes of the slice: x: 2, y: 2, z: 2, core: 2. Of those that a mesh axis runs over, the one named last changes fastest.
Arguments:
- x_tok: bfloat16 [8192, 5120], P(('dep', 'row'), 'col')
- w_up: bfloat16 [5120, 13824], P('row', 'col')
- w_down: bfloat16 [13824, 5120], P('row', 'col')
- grad_out: bfloat16 [8192, 5120], P(('dep', 'row'), 'col')
Outputs:
- output 1: bfloat16 [8192, 5120], P(('dep', 'row'), 'col')
- output 2: bfloat16 [8192, 5120], P(('dep', 'row'), 'col')
- output 3: float32 [5120, 13824], P(('row', 'dep'), 'col')
- output 4: float32 [13824, 5120], P(('row', 'dep'), 'col')
All inputs are finite; a program needn't handle non-finite values.
Results may differ from the reference program's by a relative error of at most 0.00114.
Values are sent between devices in bfloat16 or wider.
A program may use at most 1 GiB of HBM per device.

```python
import math
import jax
import jax.numpy as jnp
from jax import lax

HIDDEN = 5120
FFN_DIM = 13824
TOKENS = 8192

BLOCK_ROWS = math.gcd(TOKENS, 2048)
NUM_BLOCKS = TOKENS // BLOCK_ROWS
GELU_COEF = 0.7978845608028654
CUBIC_COEF = 0.044715


def gelu_fwd(pre_act):
    inner = GELU_COEF * (pre_act + CUBIC_COEF * pre_act * pre_act * pre_act)
    return 0.5 * pre_act * (1.0 + jnp.tanh(inner))


def gelu_slope(pre_act):
    inner = GELU_COEF * (pre_act + CUBIC_COEF * pre_act * pre_act * pre_act)
    tanh_val = jnp.tanh(inner)
    return 0.5 * (1.0 + tanh_val) + 0.5 * pre_act * (1.0 - tanh_val * tanh_val) * GELU_COEF * (1.0 + 3.0 * CUBIC_COEF * pre_act * pre_act)


def setup_inputs(seed: int = 0) -> dict:
    root_key = jax.random.key(seed)
    key_x, key_up, key_down, key_g = jax.random.split(root_key, 4)
    x_tok = jax.random.normal(key_x, (TOKENS, HIDDEN), jnp.float32).astype(jnp.bfloat16)
    w_up = (jax.random.normal(key_up, (HIDDEN, FFN_DIM), jnp.float32) * HIDDEN ** -0.5).astype(jnp.bfloat16)
    w_down = (jax.random.normal(key_down, (FFN_DIM, HIDDEN), jnp.float32) * FFN_DIM ** -0.5).astype(jnp.bfloat16)
    grad_out = jax.random.normal(key_g, (TOKENS, HIDDEN), jnp.float32).astype(jnp.bfloat16)
    return {"x_tok": x_tok, "w_up": w_up, "w_down": w_down, "grad_out": grad_out}


def reference(x_tok, w_up, w_down, grad_out):
    x_blocks = x_tok.reshape(NUM_BLOCKS, BLOCK_ROWS, HIDDEN)
    g_blocks = grad_out.reshape(NUM_BLOCKS, BLOCK_ROWS, HIDDEN)

    def block_step(acc_pair, block_in):
        dw_up_acc, dw_down_acc = acc_pair
        x_blk, g_blk = block_in
        pre_act = jnp.dot(x_blk, w_up, preferred_element_type=jnp.float32)
        hidden_act = gelu_fwd(pre_act).astype(jnp.bfloat16)
        y_blk = jnp.dot(hidden_act, w_down, preferred_element_type=jnp.float32).astype(jnp.bfloat16)
        d_act = jnp.dot(g_blk, w_down.T, preferred_element_type=jnp.float32)
        d_pre = (d_act * gelu_slope(pre_act)).astype(jnp.bfloat16)
        dx_blk = jnp.dot(d_pre, w_up.T, preferred_element_type=jnp.float32).astype(jnp.bfloat16)
        dw_up_acc = dw_up_acc + jnp.dot(x_blk.T, d_pre, preferred_element_type=jnp.float32)
        dw_down_acc = dw_down_acc + jnp.dot(hidden_act.T, g_blk, preferred_element_type=jnp.float32)
        return (dw_up_acc, dw_down_acc), (y_blk, dx_blk)

    init_acc = (jnp.zeros((HIDDEN, FFN_DIM), jnp.float32), jnp.zeros((FFN_DIM, HIDDEN), jnp.float32))
    (dw_up, dw_down), (y_blocks, dx_blocks) = lax.scan(block_step, init_acc, (x_blocks, g_blocks))
    return y_blocks.reshape(TOKENS, HIDDEN), dx_blocks.reshape(TOKENS, HIDDEN), dw_up, dw_down
```

```python
import jax
import jax.numpy as jnp
from jax import lax
from jax.sharding import PartitionSpec as P


GELU_COEF = 0.7978845608028654
CUBIC_COEF = 0.044715


CHUNKS = (((0, 640), (1792, 2304)), ((640, 1152), (2304, 2944)), ((1152, 1792), (2944, 3456)))
SPLIT = (640, 512, 576)
HALF = 3456


def gelu_and_slope(u):
    inner = GELU_COEF * (u + CUBIC_COEF * u * u * u)
    t = jnp.tanh(inner)
    act = 0.5 * u * (1.0 + t)
    slope = 0.5 * (1.0 + t) + 0.5 * u * (1.0 - t * t) * GELU_COEF * (1.0 + 3.0 * CUBIC_COEF * u * u)
    return act, slope


def dot(a, b, ca, cb):
    return lax.dot_general(a, b, (((ca,), (cb,)), ((), ())), preferred_element_type=jnp.float32)


def solution(mesh):
    act_spec = P(("dep", "row"), "col")
    wgt_spec = P("row", "col")
    grad_spec = P(("row", "dep"), "col")

    def flip(v, j):
        return lax.ppermute(v, "row", [(r, r ^ j) for r in range(4)])

    def flip_y(v):
        return lax.ppermute(v, "col", [(0, 1), (1, 0)])

    def move_z(v, pairs=((0, 1), (1, 0))):
        return lax.ppermute(v, "dep", pairs)

    def cat(parts, axis):
        return jnp.concatenate(parts, axis=axis)

    def local_block(x_loc, w1_loc, w2_loc, g_loc):
        d, y, r = lax.axis_index("dep"), lax.axis_index("col"), lax.axis_index("row")
        x, c = r // 2, r % 2
        diag = x == y
        hr = w1_loc.shape[0]
        hh = hr // 2

        def by_core(a, b):
            return jnp.where(c == 0, cat([a, b], 0), cat([b, a], 0))

        x_y = flip_y(x_loc)
        g_y = flip_y(g_loc)
        x_nat = jnp.where(y == 0, cat([x_loc, x_y], 1), cat([x_y, x_loc], 1))

        def x_half(j, h):
            return lax.dynamic_slice_in_dim(x_nat, (r ^ j) * hr + h * hh, hh, axis=1)

        x_mine = [x_half(j, d) for j in range(4)]
        x_other = [x_half(j, 1 - d) for j in range(4)]
        x_rel = cat([lax.dynamic_slice_in_dim(x_nat, (r ^ j) * hr, hr, axis=1) for j in (0, 1)] + [x_mine[2], x_other[2], x_mine[3], x_other[3]], 1)
        got = [cat([x_mine[j], x_other[j]], 1) for j in range(4)]
        got = [got[0]] + [flip(got[j], j) for j in (1, 2, 3)]
        x_mine = cat([v[:, :hh] for v in got], 0)
        x_other = cat([v[:, hh:] for v in got], 0)
        g_1, g_2 = flip(g_loc, 1), flip(g_loc, 2)
        g_lay = cat([g_loc, g_1, g_2, flip(g_2, 1)], 0)

        y_acc = dx_near = dx_far = None
        dw1, dw2 = [], []
        for k in range(3):
            near = cat([w1_loc[:, base + a : base + b] for base in (0, HALF) for a, b in CHUNKS[k]], 1)
            half = flip(lax.dynamic_slice_in_dim(near, d * hh, hh, axis=0), 2)
            far = cat([half, move_z(half)], 0)
            w1_near = cat([near, flip(near, 1)], 0)
            w1_far = cat([far, flip(far, 1)], 0)
            n0 = cat([w2_loc[a:b] for a, b in CHUNKS[k]], 0)
            size = n0.shape[0] // 2
            half = flip(lax.dynamic_slice_in_dim(n0, d * size, size, axis=0), 2)
            rest = move_z(half)
            f0 = jnp.where(d == 0, cat([half, rest], 0), cat([rest, half], 0))
            n1, f1 = flip(n0, 1), flip(f0, 1)
            cross = flip_y(jnp.where(diag, f0, n0))
            w2_there = by_core(cross, flip(cross, 1))
            w2_here = by_core(jnp.where(diag, n0, f0), jnp.where(diag, n1, f1))
            u = dot(x_rel, cat([w1_near, w1_far], 0), 1, 0)
            act32, slope = gelu_and_slope(u)
            act = act32.astype(jnp.bfloat16)
            d_act = dot(g_loc, w2_here, 1, 1) + dot(g_y, w2_there, 1, 1)
            d_pre = (d_act * slope).astype(jnp.bfloat16)
            part = dot(d_pre, w1_near, 1, 1)
            dx_near = part if dx_near is None else dx_near + part
            part = dot(d_pre, w1_far, 1, 1)
            dx_far = part if dx_far is None else dx_far + part
            p_2 = flip(d_pre, 2)
            d_lay = cat([d_pre, flip(d_pre, 1), p_2, flip(p_2, 1)], 0)
            d_lay = lax.optimization_barrier(d_lay)
            back = move_z(dot(x_other, d_lay, 0, 0))
            dw1.append(dot(x_mine, d_lay, 0, 0) + back)
            act_y = flip_y(act)
            width = act.shape[1] // 2
            a_rel = []
            for v in (jnp.where(diag, act, act_y), jnp.where(diag, act_y, act)):
                lo, hi = v[:, :width], v[:, width:]
                a_rel += [jnp.where(c == 0, lo, hi), jnp.where(c == 0, hi, lo)]
            part = dot(cat(a_rel, 1), cat([n0, n1, f0, f1], 0), 1, 0)
            y_acc = part if y_acc is None else y_acc + part
            a_lay = cat([a_rel[0]] + [flip(a_rel[j], j) for j in (1, 2, 3)], 0)
            s = SPLIT[k]
            first, second = dot(a_lay[:, :s], g_lay, 0, 0), dot(a_lay[:, s:], g_lay, 0, 0)
            dw2.append((first + move_z(first, [(1, 0)]), second + move_z(second, [(0, 1)])))

        dx_other, dx_mine = jnp.where(diag, dx_far, dx_near), jnp.where(diag, dx_near, dx_far)
        dx_rel = (dx_mine + flip_y(dx_other)).astype(jnp.bfloat16)
        turn = jnp.where(diag, 0, d)
        dx = cat([lax.dynamic_slice_in_dim(dx_rel, (((q >> 1) ^ c) * 2 + ((q & 1) ^ turn)) * hh, hh, axis=1) for q in range(4)], 1)
        cols = []
        for k in range(3):
            width = dw1[k].shape[1] // 2
            s = CHUNKS[k][0][1] - CHUNKS[k][0][0]
            for b in range(2):
                cols.append((b * HALF + CHUNKS[k][0][0], dw1[k][:, b * width : b * width + s]))
                cols.append((b * HALF + CHUNKS[k][1][0], dw1[k][:, b * width + s : (b + 1) * width]))
        dw1_out = cat([v for _, v in sorted(cols, key=lambda p: p[0])], 1)
        (a0, b0), (a1, b1), (a2, b2) = dw2
        dw2_out = jnp.where(d == 0, cat([a0, a1, a2], 0), cat([b2[:64], b0, b1, b2[64:]], 0))
        return y_acc.astype(jnp.bfloat16), dx, dw1_out, dw2_out

    return jax.shard_map(local_block, mesh=mesh, in_specs=(act_spec, wgt_spec, wgt_spec, act_spec), out_specs=(act_spec, act_spec, grad_spec, grad_spec), check_vma=False)
```
